32 devices in a mesh: member: 2 (over y), tile: 4 (over z), row: 2 (over x), lev: 2 (over core).
Axes of the slice: x: 2, y: 2, z: 4, core: 2. Of those that a mesh axis runs over, the one named last changes fastest.
Arguments:
- thickness: float32 [128, 64, 256], P(('member', 'lev'), 'tile', 'row'), parts along dimension 0, may hold values from 0.24 to 14.91
- zonal_wind: float32 [128, 64, 256], P(('member', 'lev'), 'tile', 'row'), parts along dimension 0, may hold values from -1.8 to 1.8
- merid_wind: float32 [128, 64, 256], P(('member', 'lev'), 'tile', 'row'), parts along dimension 0, may hold values from -1.8 to 1.8
- pert_codes: int32 [128, 256], P(('member', 'tile'), 'row'), parts along dimension 0, may hold values from 0 to 1073741823
Outputs:
- thick_out: float32 [128, 64, 256], P(('member', 'lev'), 'tile', 'row'), parts along dimension 0
- zonal_out: float32 [128, 64, 256], P(('member', 'lev'), 'tile', 'row'), parts along dimension 0
- merid_out: float32 [128, 64, 256], P(('member', 'lev'), 'tile', 'row'), parts along dimension 0
The draws below stay inside these ranges and needn't reach their ends.
There are 2 independent parts, one for each index of `member`. The reference program is written for one: setup_inputs(seed, part) draws one part's arguments, and reference() takes and returns one part's arrays. A program takes and returns all parts, laid end to end along the dimension named above; each array names one. Nothing has to cross between parts.
All inputs are finite; a program needn't handle non-finite values.
Results may differ from the reference program's by a relative error of at most 0.0003.
Values sent between devices are 32-bit elements; how exact they have to be, the bound alone decides.
A program may use at most 64 MiB of HBM per device.

```python
import math
import jax
import jax.numpy as jnp
from jax import lax

NZ = 64
NSUB = 4
NX = 64
NY = 256


def draw_thickness(key, part):
    scale_key = jax.random.fold_in(key, 11)
    rough_key = jax.random.fold_in(key, 23)
    region_draw = jax.random.uniform(scale_key, (8, 2), jnp.float32, 0.0, 1.0)
    region_scale = jnp.exp(math.log(0.35) + math.log(10.0) * region_draw)
    region_first = (jnp.arange(NX) * 8 // NX).astype(jnp.int32)
    region_second = (jnp.arange(NY) * 2 // NY).astype(jnp.int32)
    cell_scale = jnp.take(jnp.take(region_scale, region_first, axis=0), region_second, axis=1)
    across = jnp.arange(NX).astype(jnp.float32) / max(NX - 1, 1)
    base = (1.0 + 2.0 * across[:, None]) * cell_scale
    rough = jax.random.uniform(rough_key, (NZ, NX, NY), jnp.float32, -0.35, 0.35)
    return (base[None] * jnp.exp(rough)).astype(jnp.float32)


def place_ends(array, stream_key, smallest, high):
    longest = array.shape.index(max(array.shape))
    spots = []
    for shift in (0, 1):
        where = [jax.random.randint(jax.random.fold_in(stream_key, axis), (), 0, length) for axis, length in enumerate(array.shape)]
        where[longest] = (where[longest] + shift) % array.shape[longest]
        spots.append(tuple(where))
    return array.at[spots[0]].set(smallest).at[spots[1]].set(high)


def shard_levels(key, extent, cuts, least, high):
    level = 1.0
    for position, blocks in cuts:
        draws = jax.random.uniform(jax.random.fold_in(jax.random.fold_in(key, 6), position), (blocks,), jnp.float32, least / len(cuts), high / len(cuts))
        level = level * jnp.repeat(jnp.exp(draws), extent[position] // blocks).reshape((-1,) + (1,) * (len(extent) - 1 - position))
    return level


def centred(rng, extent, deviation, bound, shards=(), held_as=jnp.bfloat16):
    loudness = shard_levels(rng, extent, shards, -0.22, 0.18) if shards else 1.0
    drawn = jax.random.normal(rng, extent, jnp.float32) * deviation * loudness
    return jnp.minimum(jnp.maximum(drawn, -bound), bound).astype(held_as)


def setup_inputs(seed: int = 0, part: int = 0) -> dict:
    splits = jax.random.split(jax.random.key(seed), 5)
    part_splits = jax.random.split(jax.random.fold_in(splits[4], part), 5)
    thickness = draw_thickness(jax.random.fold_in(jax.random.fold_in(splits[4], part), 71), part)
    zonal_wind = centred(part_splits[1], (NZ, NX, NY), 0.3, 1.8, ((0, 2), (1, 4), (2, 2)), jnp.float32)
    merid_wind = centred(part_splits[2], (NZ, NX, NY), 0.3, 1.8, ((0, 2), (1, 4), (2, 2)), jnp.float32)
    pert_codes = place_ends(jax.random.randint(part_splits[3], (NX, NY), 0, 1073741824), jax.random.fold_in(part_splits[3], 1), 0, 1073741823).astype(jnp.int32)
    return dict(thickness=thickness, zonal_wind=zonal_wind, merid_wind=merid_wind, pert_codes=pert_codes)


CFL_NUMBER = 0.8

def advance(stacked, half_step):
    height = stacked[0]
    zonal = stacked[1]
    merid = stacked[2]
    zonal_new = zonal[:, 1:-1, 1:-1] - half_step * (height[:, 2:, 1:-1] - height[:, :-2, 1:-1])
    merid_new = merid[:, 1:-1, 1:-1] - half_step * (height[:, 1:-1, 2:] - height[:, 1:-1, :-2])
    centre = height[:, 1:-1, 1:-1]
    flux_east = centre * zonal_new
    flux_north = centre * merid_new
    height_new = centre[:, 1:-1, 1:-1] - half_step * (flux_east[:, 2:, 1:-1] - flux_east[:, :-2, 1:-1] + (flux_north[:, 1:-1, 2:] - flux_north[:, 1:-1, :-2]))
    return jnp.stack([height_new, zonal_new[:, 1:-1, 1:-1], merid_new[:, 1:-1, 1:-1]])

def reference(thickness, zonal_wind, merid_wind, pert_codes):
    bump = 2.0 * (pert_codes % 4096).astype(jnp.float32) / 4095.0
    raised = thickness + bump[None]
    peak = jnp.max(raised)
    base_mass = jnp.sum(thickness)
    raised_mass = jnp.sum(raised)
    height = raised * (base_mass / raised_mass)
    half_step = 0.5 * CFL_NUMBER / jnp.sqrt(peak)
    state = jnp.stack([height, zonal_wind, merid_wind])
    for substep in range(NSUB):
        padded = jnp.pad(state, ((0, 0), (0, 0), (2, 2), (2, 2)), mode='wrap')
        state = advance(padded, half_step)
    height = state[0]
    zonal = state[1]
    merid = state[2]
    total = lax.optimization_barrier(jnp.sum(height, 0))
    tops = jnp.cumsum(height, 0) - height
    levels = height.shape[0]

    def integral(mark):
        target = total * (mark / levels)
        over = jnp.clip(target[None] - tops, 0.0, height)
        return (lax.optimization_barrier(jnp.sum(zonal * over, 0)), lax.optimization_barrier(jnp.sum(merid * over, 0)))
    marks = jnp.arange(levels + 1).astype(jnp.int32).astype(jnp.float32)
    zonal_sum, merid_sum = lax.map(integral, marks)
    layer = total / levels
    thick_out = jnp.broadcast_to(layer, (levels,) + layer.shape)
    zonal_out = (zonal_sum[1:] - zonal_sum[:-1]) / layer
    merid_out = (merid_sum[1:] - merid_sum[:-1]) / layer
    return (thick_out, zonal_out, merid_out)
```

```python
import jax
import jax.numpy as jnp
from jax import lax
from jax.experimental import pallas as pl
from jax.experimental.pallas import tpu as pltpu
from jax.sharding import PartitionSpec as P

NSUB = 4
CFL_NUMBER = 0.8
RIM = 2 * NSUB
SUB = 8
MESH = pl.DeviceIdType.MESH


def make_kernel(T, R, V, L, X, Y):
    NB = X // SUB
    LG = L // SUB
    XP = X + 2 * RIM
    sides = (1,) if R == 2 else (1, R - 1)
    NS = len(sides)
    WIN = 2 * RIM
    offsets = set()
    for d in range(1, T):
        offsets.add((d, 0, 0))
    for r in range(R):
        for v in range(V):
            offsets.add((0, r, v))
    for r in (1, R - 1):
        for t in (1, T - 1):
            offsets.add((t, r, 0))
    offsets.discard((0, 0, 0))
    offsets = sorted(offsets)
    group = [(r, v) for r in range(R) for v in range(V)]
    peers = [p for p in group if p != (0, 0)]
    levels = V * L
    marks = L + 1
    block = 11 if marks % 11 == 0 else marks

    def kernel(t_ref, z_ref, m_ref, c_ref, th_ref, zo_ref, mo_ref,
               bump, pack, rim_pack, rim, rim_codes, part1, part2, fin, tops,
               s_part1, r_part1, s_part2, r_part2, s_row, r_row, s_cor, r_cor,
               s_rim, r_rim, s_code, r_code, s_lev, r_lev):
        me_t = lax.axis_index("tile")
        me_r = lax.axis_index("row")
        me_v = lax.axis_index("lev")

        def dev(dt, dr, dv):
            return {
                "tile": lax.rem(me_t + dt, T),
                "row": lax.rem(me_r + dr, R),
                "lev": lax.rem(me_v + dv, V),
            }

        def remote(src, dst, send, recv, where):
            return pltpu.make_async_remote_copy(
                src_ref=src, dst_ref=dst, send_sem=send, recv_sem=recv,
                device_id=where, device_id_type=MESH)

        barrier = pltpu.get_barrier_semaphore()
        for o in offsets:
            pl.semaphore_signal(barrier, inc=1, device_id=dev(*o), device_id_type=MESH)

        lane = lax.broadcasted_iota(jnp.int32, (SUB, Y), 1)
        sub = lax.broadcasted_iota(jnp.int32, (SUB, Y), 0)
        fields = (t_ref, z_ref, m_ref)
        flat = [f.reshape(L * X, Y) for f in fields]

        def bump_of(codes):
            return 2.0 * (codes & 4095).astype(jnp.float32) / 4095.0

        base = jnp.zeros((SUB, Y), jnp.float32)
        risen = jnp.zeros((SUB, Y), jnp.float32)
        top = jnp.full((SUB, Y), -jnp.inf, jnp.float32)
        for b in range(NB):
            here = bump_of(c_ref[b * SUB:(b + 1) * SUB, :])
            bump[RIM + b * SUB:RIM + (b + 1) * SUB, :] = here
            for k in range(L):
                t = t_ref[k, b * SUB:(b + 1) * SUB, :]
                up = t + here
                base = base + t
                risen = risen + up
                top = jnp.maximum(top, up)
        base = jnp.sum(base, 0, keepdims=True)
        risen = jnp.sum(risen, 0, keepdims=True)
        top = jnp.max(top, 0, keepdims=True)
        mine = jnp.where(sub == 0, base, jnp.where(sub == 1, risen, top))
        part1[me_t] = mine

        def combine(a, b):
            return jnp.where(sub < 2, a + b, jnp.maximum(a, b))

        def pack_chunk(lg, carry):
            for b in range(NB):
                for f in range(3):
                    acc = jnp.zeros((SUB, Y), jnp.float32)
                    for g in range(SUB):
                        x = b * SUB + g
                        s = flat[f][pl.ds(lg * SUB * X + x, SUB, stride=X), :]
                        if f == 0:
                            s = s + bump[RIM + x:RIM + x + 1, :]
                        s = pltpu.roll(s, (RIM + WIN * g) % Y, 1)
                        acc = jnp.where(lane // WIN == g, s, acc)
                    pack[b, lg, f] = acc
            return carry

        lax.fori_loop(0, LG, pack_chunk, 0)
        pl.semaphore_wait(barrier, len(offsets))

        part1_copies = []
        for d in range(1, T):
            c = remote(part1.at[me_t], part1.at[me_t], s_part1.at[d - 1], r_part1.at[d - 1], dev(d, 0, 0))
            c.start()
            part1_copies.append(c)
        code_copies = [
            remote(c_ref.at[pl.ds(X - RIM, RIM)], rim_codes.at[0], s_code.at[0], r_code.at[0], dev(1, 0, 0)),
            remote(c_ref.at[pl.ds(0, RIM)], rim_codes.at[1], s_code.at[1], r_code.at[1], dev(T - 1, 0, 0)),
        ]
        for c in code_copies:
            c.start()
        pack_copies = []
        for n, dr in enumerate(sides):
            pack_copies.append(remote(pack.at[NB - 1], rim_pack.at[n, 0], s_cor.at[n, 0], r_cor.at[n, 0], dev(1, dr, 0)))
            pack_copies.append(remote(pack.at[0], rim_pack.at[n, NB + 1], s_cor.at[n, 1], r_cor.at[n, 1], dev(T - 1, dr, 0)))
            pack_copies.append(remote(pack, rim_pack.at[n, pl.ds(1, NB)], s_row.at[n], r_row.at[n], dev(0, dr, 0)))
        for c in pack_copies:
            c.start()

        def rim_copies(lg):
            out = []
            for f in range(3):
                for way, first, dt in ((0, X - RIM, 1), (1, 0, T - 1)):
                    out.append(remote(
                        fields[f].at[pl.ds(lg * SUB, SUB), pl.ds(first, RIM)],
                        rim.at[way, lg, f], s_rim.at[way, lg, f], r_rim.at[way, lg, f],
                        dev(dt, 0, 0)))
            return out

        for lg in range(LG):
            for c in rim_copies(lg):
                c.start()

        for c in part1_copies:
            c.wait()
        total = part1[0]
        for d in range(1, T):
            total = combine(total, part1[d])
        slot = me_r * V + me_v
        part2[slot] = total
        part2_copies = []
        for n, (r, v) in enumerate(peers):
            c = remote(part2.at[slot], part2.at[slot], s_part2.at[n], r_part2.at[n], dev(0, r, v))
            c.start()
            part2_copies.append(c)
        for c in code_copies:
            c.wait()
        bump[0:RIM, :] = bump_of(rim_codes[0])
        bump[RIM + X:XP, :] = bump_of(rim_codes[1])
        for c in part2_copies:
            c.wait()
        total = part2[0]
        for n in range(1, R * V):
            total = combine(total, part2[n])
        base_all = jnp.sum(total[0:1, :], 1, keepdims=True)
        risen_all = jnp.sum(total[1:2, :], 1, keepdims=True)
        peak = jnp.max(total[2:3, :], 1, keepdims=True)
        factor = base_all / risen_all
        half = 0.5 * CFL_NUMBER / jnp.sqrt(peak)
        factor = jnp.broadcast_to(factor, (SUB, 2 * Y))
        half = jnp.broadcast_to(half, (SUB, 2 * Y))
        for c in pack_copies:
            c.wait()

        def lev_copies(lg):
            place = fin.at[me_v * LG + lg]
            return [
                remote(place, place, s_lev.at[v - 1, lg], r_lev.at[v - 1, lg], dev(0, 0, v))
                for v in range(1, V)
            ]

        def chunk(lg, carry):
            for c in rim_copies(lg):
                c.wait()
            low = [rim.at[0, lg, f].reshape(SUB * RIM, Y) for f in range(3)]
            high = [rim.at[1, lg, f].reshape(SUB * RIM, Y) for f in range(3)]

            def load(f, i):
                if i < RIM:
                    main = low[f][pl.ds(i, SUB, stride=RIM), :]
                elif i < RIM + X:
                    main = flat[f][pl.ds(lg * SUB * X + i - RIM, SUB, stride=X), :]
                else:
                    main = high[f][pl.ds(i - RIM - X, SUB, stride=RIM), :]
                if f == 0:
                    main = main + bump[i:i + 1, :]
                b, g = i // SUB, i % SUB
                shift = (2 * Y - RIM - WIN * g) % Y
                wing = pltpu.roll(rim_pack[0, b, lg, f], shift, 1)
                if NS == 2:
                    other = pltpu.roll(rim_pack[1, b, lg, f], shift, 1)
                    wing = jnp.where(lane < Y // 2, other, wing)
                both = jnp.concatenate([main, wing], 1)
                return both * factor if f == 0 else both

            memo = {}

            def keep(key, make):
                if key not in memo:
                    memo[key] = make()
                return memo[key]

            def ddy(a):
                return pltpu.roll(a, 2 * Y - 1, 1) - pltpu.roll(a, 1, 1)

            def H(s, i):
                if s == 0:
                    return keep(("h", 0, i), lambda: load(0, i))
                return keep(("h", s, i), lambda: H(s - 1, i) - half * (
                    (FE(s, i + 1) - FE(s, i - 1)) + ddy(H(s - 1, i) * W2(s, i))))

            def W1(s, i):
                if s == 0:
                    return keep(("u", 0, i), lambda: load(1, i))
                return keep(("u", s, i), lambda: W1(s - 1, i) - half * (H(s - 1, i + 1) - H(s - 1, i - 1)))

            def W2(s, i):
                if s == 0:
                    return keep(("v", 0, i), lambda: load(2, i))
                return keep(("v", s, i), lambda: W2(s - 1, i) - half * ddy(H(s - 1, i)))

            def FE(s, i):
                return keep(("e", s, i), lambda: H(s - 1, i) * W1(s, i))

            mine_at = me_v * LG + lg
            for x in range(X):
                i = x + RIM
                fin[mine_at, 0, pl.ds(x, SUB, stride=X), :] = H(NSUB, i)[:, :Y]
                fin[mine_at, 1, pl.ds(x, SUB, stride=X), :] = W1(NSUB, i)[:, :Y]
                fin[mine_at, 2, pl.ds(x, SUB, stride=X), :] = W2(NSUB, i)[:, :Y]
            for c in lev_copies(lg):
                c.start()
            return carry

        lax.fori_loop(0, LG, chunk, 0)
        for lg in range(LG):
            for c in lev_copies(lg):
                c.wait()

        first = me_v * L
        for b in range(NB):
            rows = slice(b * SUB, (b + 1) * SUB)

            def prefix(c, run):
                for j in range(SUB):
                    tops[c * SUB + j] = run
                    run = run + fin[c, 0, j * X + b * SUB:j * X + (b + 1) * SUB, :]
                return run

            total = lax.fori_loop(0, V * LG, prefix, jnp.zeros((SUB, Y), jnp.float32))
            layer = total / levels
            last = None
            for start in range(0, marks, block):
                goals = [
                    total * ((first + start + n).astype(jnp.float32) / levels)
                    for n in range(block)
                ]

                def gather(c, sums):
                    sums = list(sums)
                    for j in range(SUB):
                        at = slice(j * X + b * SUB, j * X + (b + 1) * SUB)
                        h = fin[c, 0, at, :]
                        z = fin[c, 1, at, :]
                        m = fin[c, 2, at, :]
                        t = tops[c * SUB + j]
                        for n in range(block):
                            over = jnp.minimum(jnp.maximum(goals[n] - t, 0.0), h)
                            sums[2 * n] = sums[2 * n] + z * over
                            sums[2 * n + 1] = sums[2 * n + 1] + m * over
                    return tuple(sums)

                zero = jnp.zeros((SUB, Y), jnp.float32)
                sums = lax.fori_loop(0, V * LG, gather, (zero,) * (2 * block))
                for n in range(block):
                    now = (sums[2 * n], sums[2 * n + 1])
                    if last is not None:
                        k = start + n - 1
                        th_ref[k, rows, :] = layer
                        zo_ref[k, rows, :] = (now[0] - last[0]) / layer
                        mo_ref[k, rows, :] = (now[1] - last[1]) / layer
                    last = now

    vm = lambda *s: pltpu.VMEM(s, jnp.float32)
    dma = lambda *s: pltpu.SemaphoreType.DMA(s)
    scratch = [
        vm(XP, Y),
        vm(NB, LG, 3, SUB, Y),
        vm(NS, NB + 2, LG, 3, SUB, Y),
        vm(2, LG, 3, SUB, RIM, Y),
        pltpu.VMEM((2, RIM, Y), jnp.int32),
        vm(T, SUB, Y),
        vm(R * V, SUB, Y),
        vm(V * LG, 3, SUB * X, Y),
        vm(levels, SUB, Y),
        dma(T - 1), dma(T - 1), dma(R * V - 1), dma(R * V - 1),
        dma(NS), dma(NS), dma(NS, 2), dma(NS, 2),
        dma(2, LG, 3), dma(2, LG, 3), dma(2), dma(2),
        dma(V - 1, LG), dma(V - 1, LG),
    ]
    return kernel, scratch


def solution(mesh):
    T, R, V = mesh.shape["tile"], mesh.shape["row"], mesh.shape["lev"]

    def local(thickness, zonal_wind, merid_wind, pert_codes):
        L, X, Y = thickness.shape
        kernel, scratch = make_kernel(T, R, V, L, X, Y)
        spec = pl.BlockSpec(memory_space=pltpu.VMEM)
        out = jax.ShapeDtypeStruct((L, X, Y), jnp.float32)
        return pl.pallas_call(
            kernel,
            out_shape=(out,) * 3,
            in_specs=[spec] * 4,
            out_specs=(spec,) * 3,
            scratch_shapes=scratch,
            compiler_params=pltpu.CompilerParams(collective_id=0, has_side_effects=True),
        )(thickness, zonal_wind, merid_wind, pert_codes)

    field = P(("member", "lev"), "tile", "row")
    return jax.shard_map(
        local, mesh=mesh,
        in_specs=(field, field, field, P(("member", "tile"), "row")),
        out_specs=(field,) * 3, check_vma=False)
```

```python
import jax
import jax.numpy as jnp
from jax import lax
from jax.experimental import pallas as pl
from jax.experimental.pallas import tpu as pltpu
from jax.sharding import PartitionSpec as P

NSUB = 4
CFL_NUMBER = 0.8
RIM = 2 * NSUB
SUB = 8
FIRST = 1
VMEM = 65466368
MESH = pl.DeviceIdType.MESH


def make_kernel(T, R, V, L, X, Y):
    NB = X // SUB
    LG = L // SUB
    XP = X + 2 * RIM
    sides = (1,) if R == 2 else (1, R - 1)
    NS = len(sides)
    WIN = 2 * RIM
    offsets = set()
    for d in range(1, T):
        offsets.add((d, 0, 0))
    for r in range(R):
        for v in range(V):
            offsets.add((0, r, v))
    for r in (1, R - 1):
        for t in (1, T - 1):
            offsets.add((t, r, 0))
    offsets.discard((0, 0, 0))
    offsets = sorted(offsets)
    group = [(r, v) for r in range(R) for v in range(V)]
    peers = [p for p in group if p != (0, 0)]
    levels = V * L
    marks = L + 1
    block = 11 if marks % 11 == 0 else marks

    def kernel(t_in, z_in, m_in, c_in, out,
               t_ref, z_ref, m_ref, c_ref, s_in, bump, pack, rim_pack, rim, rim_codes, part1, part2, own, s_out,
               s_part1, r_part1, s_part2, r_part2, s_row, r_row, s_cor, r_cor,
               s_rim, r_rim, s_code, r_code, s_lev, r_lev):
        me_t = lax.axis_index("tile")
        me_r = lax.axis_index("row")
        me_v = lax.axis_index("lev")

        def dev(dt, dr, dv):
            return {
                "tile": lax.rem(me_t + dt, T),
                "row": lax.rem(me_r + dr, R),
                "lev": lax.rem(me_v + dv, V),
            }

        def remote(src, dst, send, recv, where):
            return pltpu.make_async_remote_copy(
                src_ref=src, dst_ref=dst, send_sem=send, recv_sem=recv,
                device_id=where, device_id_type=MESH)

        barrier = pltpu.get_barrier_semaphore()
        for o in offsets:
            pl.semaphore_signal(barrier, inc=1, device_id=dev(*o), device_id_type=MESH)

        loads = [
            pltpu.make_async_copy(a, b, s_in.at[n])
            for n, (a, b) in enumerate(((t_in, t_ref), (z_in, z_ref), (m_in, m_ref), (c_in, c_ref)))
        ]
        for c in loads:
            c.start()

        lane = lax.broadcasted_iota(jnp.int32, (SUB, Y), 1)
        sub = lax.broadcasted_iota(jnp.int32, (SUB, Y), 0)
        fields = (t_ref, z_ref, m_ref)
        flat = [f.reshape(L * X, Y) for f in fields]

        def rim_copies(lg):
            out = []
            for f in range(3):
                for way, first, dt in ((0, X - RIM, 1), (1, 0, T - 1)):
                    out.append(remote(
                        fields[f].at[pl.ds(lg * SUB, SUB), pl.ds(first + (f if way == 0 else 0), RIM - f)],
                        rim.at[way, lg, f, :, pl.ds(f if way == 0 else 0, RIM - f)], s_rim.at[way, lg, f], r_rim.at[way, lg, f],
                        dev(dt, 0, 0)))
            return out

        for c in loads:
            c.wait()
        pl.semaphore_wait(barrier, len(offsets))
        for lg in range(FIRST):
            for c in rim_copies(lg):
                c.start()
        code_copies = [
            remote(c_ref.at[pl.ds(X - RIM, RIM)], rim_codes.at[0], s_code.at[0], r_code.at[0], dev(1, 0, 0)),
            remote(c_ref.at[pl.ds(0, RIM)], rim_codes.at[1], s_code.at[1], r_code.at[1], dev(T - 1, 0, 0)),
        ]
        for c in code_copies:
            c.start()

        def bump_of(codes):
            return 2.0 * (codes & 4095).astype(jnp.float32) / 4095.0

        base = jnp.zeros((SUB, Y), jnp.float32)
        risen = jnp.zeros((SUB, Y), jnp.float32)
        top = jnp.full((SUB, Y), -jnp.inf, jnp.float32)
        for b in range(NB):
            here = bump_of(c_ref[b * SUB:(b + 1) * SUB, :])
            bump[RIM + b * SUB:RIM + (b + 1) * SUB, :] = here
            for k in range(L):
                t = t_ref[k, b * SUB:(b + 1) * SUB, :]
                up = t + here
                base = base + t
                risen = risen + up
                top = jnp.maximum(top, up)
        base = jnp.sum(base, 0, keepdims=True)
        risen = jnp.sum(risen, 0, keepdims=True)
        top = jnp.max(top, 0, keepdims=True)
        mine = jnp.where(sub == 0, base, jnp.where(sub == 1, risen, top))
        part1[me_t] = mine

        def combine(a, b):
            return jnp.where(sub < 2, a + b, jnp.maximum(a, b))

        part1_copies = []
        for d in range(1, T):
            c = remote(part1.at[me_t], part1.at[me_t], s_part1.at[d - 1], r_part1.at[d - 1], dev(d, 0, 0))
            c.start()
            part1_copies.append(c)
        def pack_chunk(lg, carry):
            for b in range(NB):
                for f in range(3):
                    acc = jnp.zeros((SUB, Y), jnp.float32)
                    for g in range(SUB):
                        x = b * SUB + g
                        s = flat[f][pl.ds(lg * SUB * X + x, SUB, stride=X), :]
                        if f == 0:
                            s = s + bump[RIM + x:RIM + x + 1, :]
                        s = pltpu.roll(s, (RIM + WIN * g) % Y, 1)
                        acc = jnp.where(lane // WIN == g, s, acc)
                    pack[b, lg, f] = acc
            return carry

        lax.fori_loop(0, LG, pack_chunk, 0)

        pack_copies = []
        for n, dr in enumerate(sides):
            pack_copies.append(remote(pack.at[NB - 1], rim_pack.at[n, 0], s_cor.at[n, 0], r_cor.at[n, 0], dev(1, dr, 0)))
            pack_copies.append(remote(pack.at[0], rim_pack.at[n, NB + 1], s_cor.at[n, 1], r_cor.at[n, 1], dev(T - 1, dr, 0)))
            pack_copies.append(remote(pack, rim_pack.at[n, pl.ds(1, NB)], s_row.at[n], r_row.at[n], dev(0, dr, 0)))
        for c in pack_copies:
            c.start()

        for lg in range(FIRST, LG):
            for c in rim_copies(lg):
                c.start()

        for c in part1_copies:
            c.wait()
        total = part1[0]
        for d in range(1, T):
            total = combine(total, part1[d])
        slot = me_r * V + me_v
        part2[slot] = total
        part2_copies = []
        for n, (r, v) in enumerate(peers):
            c = remote(part2.at[slot], part2.at[slot], s_part2.at[n], r_part2.at[n], dev(0, r, v))
            c.start()
            part2_copies.append(c)
        for c in code_copies:
            c.wait()
        bump[0:RIM, :] = bump_of(rim_codes[0])
        bump[RIM + X:XP, :] = bump_of(rim_codes[1])
        for c in part2_copies:
            c.wait()
        total = part2[0]
        for n in range(1, R * V):
            total = combine(total, part2[n])
        base_all = jnp.sum(total[0:1, :], 1, keepdims=True)
        risen_all = jnp.sum(total[1:2, :], 1, keepdims=True)
        peak = jnp.max(total[2:3, :], 1, keepdims=True)
        factor = base_all / risen_all
        half = 0.5 * CFL_NUMBER / jnp.sqrt(peak)
        factor = jnp.broadcast_to(factor, (SUB, 2 * Y))
        half = jnp.broadcast_to(half, (SUB, 2 * Y))
        for c in pack_copies:
            c.wait()

        def lev_copies(lg):
            place = out.at[me_v * LG + lg]
            return [pltpu.make_async_copy(own.at[lg], place, s_out.at[lg])] + [
                remote(own.at[lg], place, s_lev.at[v - 1, lg], r_lev.at[v - 1, lg], dev(0, 0, v))
                for v in range(1, V)
            ]

        def chunk(lg, carry):
            for c in rim_copies(lg):
                c.wait()
            low = [rim.at[0, lg, f].reshape(SUB * RIM, Y) for f in range(3)]
            high = [rim.at[1, lg, f].reshape(SUB * RIM, Y) for f in range(3)]

            def load(f, i):
                if i < RIM:
                    main = low[f][pl.ds(i, SUB, stride=RIM), :]
                elif i < RIM + X:
                    main = flat[f][pl.ds(lg * SUB * X + i - RIM, SUB, stride=X), :]
                else:
                    main = high[f][pl.ds(i - RIM - X, SUB, stride=RIM), :]
                if f == 0:
                    main = main + bump[i:i + 1, :]
                b, g = i // SUB, i % SUB
                shift = (2 * Y - RIM - WIN * g) % Y
                wing = pltpu.roll(rim_pack[0, b, lg, f], shift, 1)
                if NS == 2:
                    other = pltpu.roll(rim_pack[1, b, lg, f], shift, 1)
                    wing = jnp.where(lane < Y // 2, other, wing)
                both = jnp.concatenate([main, wing], 1)
                return both * factor if f == 0 else both

            memo = {}

            def keep(key, make):
                if key not in memo:
                    memo[key] = make()
                return memo[key]

            def ddy(a):
                return pltpu.roll(a, 2 * Y - 1, 1) - pltpu.roll(a, 1, 1)

            def H(s, i):
                if s == 0:
                    return keep(("h", 0, i), lambda: load(0, i))
                return keep(("h", s, i), lambda: H(s - 1, i) - half * (
                    (FE(s, i + 1) - FE(s, i - 1)) + ddy(H(s - 1, i) * W2(s, i))))

            def W1(s, i):
                if s == 0:
                    return keep(("u", 0, i), lambda: load(1, i))
                return keep(("u", s, i), lambda: W1(s - 1, i) - half * (H(s - 1, i + 1) - H(s - 1, i - 1)))

            def W2(s, i):
                if s == 0:
                    return keep(("v", 0, i), lambda: load(2, i))
                return keep(("v", s, i), lambda: W2(s - 1, i) - half * ddy(H(s - 1, i)))

            def FE(s, i):
                return keep(("e", s, i), lambda: H(s - 1, i) * W1(s, i))

            for x in range(X):
                i = x + RIM
                own[lg, 0, pl.ds(x, SUB, stride=X), :] = H(NSUB, i)[:, :Y]
                own[lg, 1, pl.ds(x, SUB, stride=X), :] = W1(NSUB, i)[:, :Y]
                own[lg, 2, pl.ds(x, SUB, stride=X), :] = W2(NSUB, i)[:, :Y]
            for c in lev_copies(lg):
                c.start()
            return carry

        lax.fori_loop(0, LG, chunk, 0)
        for lg in range(LG):
            for c in lev_copies(lg):
                c.wait()

    def remap(state, th_ref, zo_ref, mo_ref, fin, tops, s_in):
        loads = [
            pltpu.make_async_copy(state.at[:, f], fin.at[:, f], s_in.at[f])
            for f in range(3)
        ]
        for c in loads:
            c.start()
        loads[0].wait()
        first = lax.axis_index("lev") * L
        for b in range(NB):
            rows = slice(b * SUB, (b + 1) * SUB)

            def prefix(c, run):
                for j in range(SUB):
                    tops[c * SUB + j] = run
                    run = run + fin[c, 0, j * X + b * SUB:j * X + (b + 1) * SUB, :]
                return run

            total = lax.fori_loop(0, V * LG, prefix, jnp.zeros((SUB, Y), jnp.float32))
            layer = total / levels
            if b == 0:
                loads[1].wait()
                loads[2].wait()
            last = None
            for start in range(0, marks, block):
                goals = [
                    total * ((first + start + n).astype(jnp.float32) / levels)
                    for n in range(block)
                ]

                def gather(c, sums):
                    sums = list(sums)
                    for j in range(SUB):
                        at = slice(j * X + b * SUB, j * X + (b + 1) * SUB)
                        h = fin[c, 0, at, :]
                        z = fin[c, 1, at, :]
                        m = fin[c, 2, at, :]
                        t = tops[c * SUB + j]
                        for n in range(block):
                            over = jnp.minimum(jnp.maximum(goals[n] - t, 0.0), h)
                            sums[2 * n] = sums[2 * n] + z * over
                            sums[2 * n + 1] = sums[2 * n + 1] + m * over
                    return tuple(sums)

                zero = jnp.zeros((SUB, Y), jnp.float32)
                sums = lax.fori_loop(0, V * LG, gather, (zero,) * (2 * block))
                for n in range(block):
                    now = (sums[2 * n], sums[2 * n + 1])
                    if last is not None:
                        k = start + n - 1
                        th_ref[k, rows, :] = layer
                        zo_ref[k, rows, :] = (now[0] - last[0]) / layer
                        mo_ref[k, rows, :] = (now[1] - last[1]) / layer
                    last = now

    vm = lambda *s: pltpu.VMEM(s, jnp.float32)
    dma = lambda *s: pltpu.SemaphoreType.DMA(s)
    scratch = [
        vm(L, X, Y), vm(L, X, Y), vm(L, X, Y),
        pltpu.VMEM((X, Y), jnp.int32),
        dma(4),
        vm(XP, Y),
        vm(NB, LG, 3, SUB, Y),
        vm(NS, NB + 2, LG, 3, SUB, Y),
        vm(2, LG, 3, SUB, RIM, Y),
        pltpu.VMEM((2, RIM, Y), jnp.int32),
        vm(T, SUB, Y),
        vm(R * V, SUB, Y),
        vm(LG, 3, SUB * X, Y), dma(LG),
        dma(T - 1), dma(T - 1), dma(R * V - 1), dma(R * V - 1),
        dma(NS), dma(NS), dma(NS, 2), dma(NS, 2),
        dma(2, LG, 3), dma(2, LG, 3), dma(2), dma(2),
        dma(V - 1, LG), dma(V - 1, LG),
    ]
    return kernel, scratch, (V * LG, 3, SUB * X, Y), remap, [vm(V * LG, 3, SUB * X, Y), vm(levels, SUB, Y), dma(3)]


def solution(mesh):
    T, R, V = mesh.shape["tile"], mesh.shape["row"], mesh.shape["lev"]

    def local(thickness, zonal_wind, merid_wind, pert_codes):
        L, X, Y = thickness.shape
        kernel, scratch, state, remap, held = make_kernel(T, R, V, L, X, Y)
        spec = pl.BlockSpec(memory_space=pltpu.VMEM)
        out = jax.ShapeDtypeStruct((L, X, Y), jnp.float32)
        columns = pl.pallas_call(
            kernel,
            out_shape=jax.ShapeDtypeStruct(state, jnp.float32),
            in_specs=[pl.BlockSpec(memory_space=pl.ANY)] * 4,
            out_specs=pl.BlockSpec(memory_space=pl.ANY),
            scratch_shapes=scratch,
            compiler_params=pltpu.CompilerParams(
                collective_id=0, has_side_effects=True, vmem_limit_bytes=VMEM),
        )(thickness, zonal_wind, merid_wind, pert_codes)
        return pl.pallas_call(
            remap,
            out_shape=(out,) * 3,
            in_specs=[pl.BlockSpec(memory_space=pl.ANY)],
            out_specs=(spec,) * 3,
            scratch_shapes=held,
            compiler_params=pltpu.CompilerParams(vmem_limit_bytes=VMEM),
        )(columns)

    field = P(("member", "lev"), "tile", "row")
    return jax.shard_map(
        local, mesh=mesh,
        in_specs=(field, field, field, P(("member", "tile"), "row")),
        out_specs=(field,) * 3, check_vma=False)
```

```python
import jax
import jax.numpy as jnp
from jax import lax
from jax.experimental import pallas as pl
from jax.experimental.pallas import tpu as pltpu
from jax.sharding import PartitionSpec as P

NSUB = 4
CFL_NUMBER = 0.8
RIM = 2 * NSUB
SUB = 8
FIRST = 1
VMEM = 65466368
MESH = pl.DeviceIdType.MESH


def make_kernel(T, R, V, L, X, Y):
    NB = X // SUB
    LG = L // SUB
    XP = X + 2 * RIM
    sides = (1,) if R == 2 else (1, R - 1)
    NS = len(sides)
    WIN = 2 * RIM
    offsets = set()
    for d in range(1, T):
        offsets.add((d, 0, 0))
    for r in range(R):
        for v in range(V):
            offsets.add((0, r, v))
    for r in (1, R - 1):
        for t in (1, T - 1):
            offsets.add((t, r, 0))
    offsets.discard((0, 0, 0))
    offsets = sorted(offsets)
    group = [(r, v) for r in range(R) for v in range(V)]
    peers = [p for p in group if p != (0, 0)]
    levels = V * L
    marks = L + 1
    block = 11 if marks % 11 == 0 else marks

    def kernel(t_in, z_in, m_in, c_in, out,
               t_ref, z_ref, m_ref, c_ref, s_in, bump, pack, rim_pack, rim, rim_codes, part1, part2, own, s_out,
               s_part1, r_part1, s_part2, r_part2, s_row, r_row, s_cor, r_cor,
               s_rim, r_rim, s_code, r_code, s_lev, r_lev):
        me_t = lax.axis_index("tile")
        me_r = lax.axis_index("row")
        me_v = lax.axis_index("lev")

        def dev(dt, dr, dv):
            return {
                "tile": lax.rem(me_t + dt, T),
                "row": lax.rem(me_r + dr, R),
                "lev": lax.rem(me_v + dv, V),
            }

        def remote(src, dst, send, recv, where):
            return pltpu.make_async_remote_copy(
                src_ref=src, dst_ref=dst, send_sem=send, recv_sem=recv,
                device_id=where, device_id_type=MESH)

        barrier = pltpu.get_barrier_semaphore()
        for o in offsets:
            pl.semaphore_signal(barrier, inc=1, device_id=dev(*o), device_id_type=MESH)

        loads = [
            pltpu.make_async_copy(a, b, s_in.at[n])
            for n, (a, b) in enumerate(((t_in, t_ref), (z_in, z_ref), (m_in, m_ref), (c_in, c_ref)))
        ]
        for c in loads:
            c.start()

        lane = lax.broadcasted_iota(jnp.int32, (SUB, Y), 1)
        sub = lax.broadcasted_iota(jnp.int32, (SUB, Y), 0)
        fields = (t_ref, z_ref, m_ref)
        flat = [f.reshape(L * X, Y) for f in fields]

        def rim_copies(lg):
            out = []
            for f in range(3):
                for way, first, dt in ((0, X - RIM, 1), (1, 0, T - 1)):
                    out.append(remote(
                        fields[f].at[pl.ds(lg * SUB, SUB), pl.ds(first + (f if way == 0 else 0), RIM - f)],
                        rim.at[way, lg, f, :, pl.ds(f if way == 0 else 0, RIM - f)], s_rim.at[way, lg, f], r_rim.at[way, lg, f],
                        dev(dt, 0, 0)))
            return out

        for c in loads:
            c.wait()
        pl.semaphore_wait(barrier, len(offsets))
        for lg in range(FIRST):
            for c in rim_copies(lg):
                c.start()
        code_copies = [
            remote(c_ref.at[pl.ds(X - RIM, RIM)], rim_codes.at[0], s_code.at[0], r_code.at[0], dev(1, 0, 0)),
            remote(c_ref.at[pl.ds(0, RIM)], rim_codes.at[1], s_code.at[1], r_code.at[1], dev(T - 1, 0, 0)),
        ]
        for c in code_copies:
            c.start()

        def bump_of(codes):
            return 2.0 * (codes & 4095).astype(jnp.float32) / 4095.0

        base = jnp.zeros((SUB, Y), jnp.float32)
        risen = jnp.zeros((SUB, Y), jnp.float32)
        top = jnp.full((SUB, Y), -jnp.inf, jnp.float32)
        for b in range(NB):
            here = bump_of(c_ref[b * SUB:(b + 1) * SUB, :])
            bump[RIM + b * SUB:RIM + (b + 1) * SUB, :] = here
            for k in range(L):
                t = t_ref[k, b * SUB:(b + 1) * SUB, :]
                up = t + here
                base = base + t
                risen = risen + up
                top = jnp.maximum(top, up)
        base = jnp.sum(base, 0, keepdims=True)
        risen = jnp.sum(risen, 0, keepdims=True)
        top = jnp.max(top, 0, keepdims=True)
        mine = jnp.where(sub == 0, base, jnp.where(sub == 1, risen, top))
        part1[me_t] = mine

        def combine(a, b):
            return jnp.where(sub < 2, a + b, jnp.maximum(a, b))

        part1_copies = []
        for d in range(1, T):
            c = remote(part1.at[me_t], part1.at[me_t], s_part1.at[d - 1], r_part1.at[d - 1], dev(d, 0, 0))
            c.start()
            part1_copies.append(c)
        def pack_chunk(lg, carry):
            for b in range(NB):
                for f in range(3):
                    acc = jnp.zeros((SUB, Y), jnp.float32)
                    for g in range(SUB):
                        x = b * SUB + g
                        s = flat[f][pl.ds(lg * SUB * X + x, SUB, stride=X), :]
                        if f == 0:
                            s = s + bump[RIM + x:RIM + x + 1, :]
                        s = pltpu.roll(s, (RIM + WIN * g) % Y, 1)
                        acc = jnp.where(lane // WIN == g, s, acc)
                    pack[b, lg, f] = acc
            return carry

        lax.fori_loop(0, LG, pack_chunk, 0)

        pack_copies = []
        for n, dr in enumerate(sides):
            pack_copies.append(remote(pack.at[NB - 1], rim_pack.at[n, 0], s_cor.at[n, 0], r_cor.at[n, 0], dev(1, dr, 0)))
            pack_copies.append(remote(pack.at[0], rim_pack.at[n, NB + 1], s_cor.at[n, 1], r_cor.at[n, 1], dev(T - 1, dr, 0)))
            pack_copies.append(remote(pack, rim_pack.at[n, pl.ds(1, NB)], s_row.at[n], r_row.at[n], dev(0, dr, 0)))
        for c in pack_copies:
            c.start()

        for lg in range(FIRST, LG):
            for c in rim_copies(lg):
                c.start()

        for c in part1_copies:
            c.wait()
        total = part1[0]
        for d in range(1, T):
            total = combine(total, part1[d])
        slot = me_r * V + me_v
        part2[slot] = total
        part2_copies = []
        for n, (r, v) in enumerate(peers):
            c = remote(part2.at[slot], part2.at[slot], s_part2.at[n], r_part2.at[n], dev(0, r, v))
            c.start()
            part2_copies.append(c)
        for c in code_copies:
            c.wait()
        bump[0:RIM, :] = bump_of(rim_codes[0])
        bump[RIM + X:XP, :] = bump_of(rim_codes[1])
        for c in part2_copies:
            c.wait()
        total = part2[0]
        for n in range(1, R * V):
            total = combine(total, part2[n])
        base_all = jnp.sum(total[0:1, :], 1, keepdims=True)
        risen_all = jnp.sum(total[1:2, :], 1, keepdims=True)
        peak = jnp.max(total[2:3, :], 1, keepdims=True)
        factor = base_all / risen_all
        half = 0.5 * CFL_NUMBER / jnp.sqrt(peak)
        factor = jnp.broadcast_to(factor, (SUB, 2 * Y))
        half = jnp.broadcast_to(half, (SUB, 2 * Y))
        for c in pack_copies:
            c.wait()

        def lev_copies(lg):
            place = out.at[me_v * LG + lg]
            return [pltpu.make_async_copy(own.at[lg], place, s_out.at[lg])] + [
                remote(own.at[lg], place, s_lev.at[v - 1, lg], r_lev.at[v - 1, lg], dev(0, 0, v))
                for v in range(1, V)
            ]

        def chunk(lg, carry):
            for c in rim_copies(lg):
                c.wait()
            low = [rim.at[0, lg, f].reshape(SUB * RIM, Y) for f in range(3)]
            high = [rim.at[1, lg, f].reshape(SUB * RIM, Y) for f in range(3)]

            def load(f, i):
                if i < RIM:
                    main = low[f][pl.ds(i, SUB, stride=RIM), :]
                elif i < RIM + X:
                    main = flat[f][pl.ds(lg * SUB * X + i - RIM, SUB, stride=X), :]
                else:
                    main = high[f][pl.ds(i - RIM - X, SUB, stride=RIM), :]
                if f == 0:
                    main = main + bump[i:i + 1, :]
                b, g = i // SUB, i % SUB
                shift = (2 * Y - RIM - WIN * g) % Y
                wing = pltpu.roll(rim_pack[0, b, lg, f], shift, 1)
                if NS == 2:
                    other = pltpu.roll(rim_pack[1, b, lg, f], shift, 1)
                    wing = jnp.where(lane < Y // 2, other, wing)
                both = jnp.concatenate([main, wing], 1)
                return both * factor if f == 0 else both

            memo = {}

            def keep(key, make):
                if key not in memo:
                    memo[key] = make()
                return memo[key]

            def ddy(a):
                return pltpu.roll(a, 2 * Y - 1, 1) - pltpu.roll(a, 1, 1)

            def H(s, i):
                if s == 0:
                    return keep(("h", 0, i), lambda: load(0, i))
                return keep(("h", s, i), lambda: H(s - 1, i) - half * (
                    (FE(s, i + 1) - FE(s, i - 1)) + ddy(H(s - 1, i) * W2(s, i))))

            def W1(s, i):
                if s == 0:
                    return keep(("u", 0, i), lambda: load(1, i))
                return keep(("u", s, i), lambda: W1(s - 1, i) - half * (H(s - 1, i + 1) - H(s - 1, i - 1)))

            def W2(s, i):
                if s == 0:
                    return keep(("v", 0, i), lambda: load(2, i))
                return keep(("v", s, i), lambda: W2(s - 1, i) - half * ddy(H(s - 1, i)))

            def FE(s, i):
                return keep(("e", s, i), lambda: H(s - 1, i) * W1(s, i))

            for x in range(X):
                i = x + RIM
                own[lg, 0, pl.ds(x, SUB, stride=X), :] = H(NSUB, i)[:, :Y]
                own[lg, 1, pl.ds(x, SUB, stride=X), :] = W1(NSUB, i)[:, :Y]
                own[lg, 2, pl.ds(x, SUB, stride=X), :] = W2(NSUB, i)[:, :Y]
            for c in lev_copies(lg):
                c.start()
            return carry

        lax.fori_loop(0, LG, chunk, 0)
        for lg in range(LG):
            for c in lev_copies(lg):
                c.wait()

    def remap(state, th_out, zo_out, mo_out, fin, tops, s_in, th_ref, zo_ref, mo_ref, s_done):
        stores = []

        def store(n, b, src, dst):
            at = (slice(None), pl.ds(b * SUB, SUB))
            c = pltpu.make_async_copy(src.at[at], dst.at[at], s_done.at[n, b])
            c.start()
            stores.append(c)

        loads = [
            pltpu.make_async_copy(state.at[:, f], fin.at[:, f], s_in.at[f])
            for f in range(3)
        ]
        for c in loads:
            c.start()
        loads[0].wait()
        first = lax.axis_index("lev") * L
        for b in range(NB):
            rows = slice(b * SUB, (b + 1) * SUB)

            def prefix(c, run):
                for j in range(SUB):
                    tops[c * SUB + j] = run
                    run = run + fin[c, 0, j * X + b * SUB:j * X + (b + 1) * SUB, :]
                return run

            total = lax.fori_loop(0, V * LG, prefix, jnp.zeros((SUB, Y), jnp.float32))
            layer = total / levels
            if b == 0:
                loads[1].wait()
                loads[2].wait()
            for k in range(L):
                th_ref[k, rows, :] = layer
            store(0, b, th_ref, th_out)
            last = None
            for start in range(0, marks, block):
                goals = [
                    total * ((first + start + n).astype(jnp.float32) / levels)
                    for n in range(block)
                ]

                def gather(c, sums):
                    sums = list(sums)
                    for j in range(SUB):
                        at = slice(j * X + b * SUB, j * X + (b + 1) * SUB)
                        h = fin[c, 0, at, :]
                        z = fin[c, 1, at, :]
                        m = fin[c, 2, at, :]
                        t = tops[c * SUB + j]
                        for n in range(block):
                            over = jnp.minimum(jnp.maximum(goals[n] - t, 0.0), h)
                            sums[2 * n] = sums[2 * n] + z * over
                            sums[2 * n + 1] = sums[2 * n + 1] + m * over
                    return tuple(sums)

                zero = jnp.zeros((SUB, Y), jnp.float32)
                sums = lax.fori_loop(0, V * LG, gather, (zero,) * (2 * block))
                for n in range(block):
                    now = (sums[2 * n], sums[2 * n + 1])
                    if last is not None:
                        k = start + n - 1
                        zo_ref[k, rows, :] = (now[0] - last[0]) / layer
                        mo_ref[k, rows, :] = (now[1] - last[1]) / layer
                    last = now
            store(1, b, zo_ref, zo_out)
            store(2, b, mo_ref, mo_out)
        for c in stores:
            c.wait()

    vm = lambda *s: pltpu.VMEM(s, jnp.float32)
    dma = lambda *s: pltpu.SemaphoreType.DMA(s)
    scratch = [
        vm(L, X, Y), vm(L, X, Y), vm(L, X, Y),
        pltpu.VMEM((X, Y), jnp.int32),
        dma(4),
        vm(XP, Y),
        vm(NB, LG, 3, SUB, Y),
        vm(NS, NB + 2, LG, 3, SUB, Y),
        vm(2, LG, 3, SUB, RIM, Y),
        pltpu.VMEM((2, RIM, Y), jnp.int32),
        vm(T, SUB, Y),
        vm(R * V, SUB, Y),
        vm(LG, 3, SUB * X, Y), dma(LG),
        dma(T - 1), dma(T - 1), dma(R * V - 1), dma(R * V - 1),
        dma(NS), dma(NS), dma(NS, 2), dma(NS, 2),
        dma(2, LG, 3), dma(2, LG, 3), dma(2), dma(2),
        dma(V - 1, LG), dma(V - 1, LG),
    ]
    return kernel, scratch, (V * LG, 3, SUB * X, Y), remap, [vm(V * LG, 3, SUB * X, Y), vm(levels, SUB, Y), dma(3), vm(L, X, Y), vm(L, X, Y), vm(L, X, Y), dma(3, NB)]


def solution(mesh):
    T, R, V = mesh.shape["tile"], mesh.shape["row"], mesh.shape["lev"]

    def local(thickness, zonal_wind, merid_wind, pert_codes):
        L, X, Y = thickness.shape
        kernel, scratch, state, remap, held = make_kernel(T, R, V, L, X, Y)
        out = jax.ShapeDtypeStruct((L, X, Y), jnp.float32)
        columns = pl.pallas_call(
            kernel,
            out_shape=jax.ShapeDtypeStruct(state, jnp.float32),
            in_specs=[pl.BlockSpec(memory_space=pl.ANY)] * 4,
            out_specs=pl.BlockSpec(memory_space=pl.ANY),
            scratch_shapes=scratch,
            compiler_params=pltpu.CompilerParams(
                collective_id=0, has_side_effects=True, vmem_limit_bytes=VMEM),
        )(thickness, zonal_wind, merid_wind, pert_codes)
        return pl.pallas_call(
            remap,
            out_shape=(out,) * 3,
            in_specs=[pl.BlockSpec(memory_space=pl.ANY)],
            out_specs=(pl.BlockSpec(memory_space=pl.ANY),) * 3,
            scratch_shapes=held,
            compiler_params=pltpu.CompilerParams(vmem_limit_bytes=VMEM),
        )(columns)

    field = P(("member", "lev"), "tile", "row")
    return jax.shard_map(
        local, mesh=mesh,
        in_specs=(field, field, field, P(("member", "tile"), "row")),
        out_specs=(field,) * 3, check_vma=False)
```
